256 devices in a mesh: row: 16 (over y, z_lo), col: 16 (over z_hi, x, core).
Axes of the slice: x: 4, y: 4, z: 8 (z_hi: 2, z_lo: 4; z = z_hi * 4 + z_lo), core: 2. Of those that a mesh axis runs over, the one named last changes fastest.
Arguments:
- archive: float32 [65536, 256], P('row'), may hold values from -6 to 6
- slab_index: int32 [12288], replicated, may hold values from 0 to 65535
- targets: float32 [12288, 256], P('col'), may hold values from -6 to 6
Outputs:
- panels: float32 [12288, 512], P('row')
- applied: float32 [12288, 256], P(('row', 'col'))
The draws below stay inside these ranges and needn't reach their ends.
Inputs may be any that keep to these rules, and one draw needn't show every extreme that they name: `slab_index`: values may repeat.
All inputs are finite; a program needn't handle non-finite values.
Results may differ from the reference program's by a relative error of at most 0.0003.
Values sent between devices are 32-bit elements; how exact they have to be, the bound alone decides.
No kernel may reach another device: no remote copies, remote signals or barrier semaphores. Data moves between devices by JAX's collectives and lax.ppermute only.
A program may use at most 64 MiB of HBM per device.

```python
import jax
import jax.numpy as jnp
from jax import lax

F = 256
ORDER = 12288
NB = 256
PANELS = 2
NT = 256
ARCHIVE = 65536
N_ROW = 16
N_COL = 16


def place_ends(array, own_key, low, high):
    dims = array.shape
    spot = [jax.random.randint(jax.random.fold_in(own_key, axis), (), 0, dims[axis]) for axis in range(len(dims))]
    array = array.at[tuple(spot)].set(low)
    longest = dims.index(max(dims))
    spot[longest] = (spot[longest] + 1) % dims[longest]
    return array.at[tuple(spot)].set(high)


def level_of(own_key, extent, split, low, top_value):
    level, own = 1.0, jax.random.fold_in(own_key, 6)
    for position, blocks in split:
        heights = jnp.exp(jax.random.uniform(jax.random.fold_in(own, position), (blocks,), jnp.float32, low / len(split), top_value / len(split)))
        level = level * jnp.repeat(heights, extent[position] // blocks).reshape([-1 if axis == position else 1 for axis in range(len(extent))])
    return level


def bell_draw(stream_key, extent, spread, bound, pieces=(), kind=jnp.bfloat16):
    drawn = jax.random.normal(stream_key, extent, jnp.float32) * spread
    if len(pieces) > 0:
        drawn = level_of(stream_key, extent, pieces, -0.22, 0.18) * drawn
    return jnp.clip(drawn, min=-bound, max=bound).astype(kind)


def setup_inputs(seed: int = 0) -> dict:
    arg_keys = jax.random.split(jax.random.key(seed), 4)
    return {
        "archive": bell_draw(arg_keys[0], (ARCHIVE, F), 1.0, 6.0, ((0, 16),), jnp.float32),
        "slab_index": place_ends(jax.random.randint(arg_keys[1], (ORDER,), 0, ARCHIVE), jax.random.fold_in(arg_keys[1], 1), 0, ARCHIVE - 1).astype(jnp.int32),
        "targets": bell_draw(arg_keys[2], (ORDER, NT), 1.0, 6.0, ((0, 16),), jnp.float32),
    }


precise = lax.Precision.HIGHEST
length_scale = 16.0
nugget = 1.0
root_five = 5.0 ** 0.5

def matern(left, right, left_ids, right_ids):
    left_sq = lax.optimization_barrier(jnp.sum(left * left, axis=1))
    right_sq = lax.optimization_barrier(jnp.sum(right * right, axis=1))
    cross = lax.dot_general(left.astype(jnp.float32), right.astype(jnp.float32), (((1,), (1,)), ((), ())), precision=precise, preferred_element_type=jnp.float32)
    squared = left_sq[:, None] + right_sq[None, :] - 2.0 * cross
    scaled = root_five * jnp.sqrt(jnp.maximum(squared, 1.0)) / length_scale
    kernel = (1.0 + scaled + scaled * scaled / 3.0) * jnp.exp(-scaled)
    return kernel + jnp.where(left_ids[:, None] == right_ids[None, :], nugget, 0.0)

def product(left, right):
    return jnp.dot(left.astype(jnp.float32), right.astype(jnp.float32), precision=precise, preferred_element_type=jnp.float32)

def outer_product(left, right):
    return lax.dot_general(left.astype(jnp.float32), right.astype(jnp.float32), (((1,), (1,)), ((), ())), precision=precise, preferred_element_type=jnp.float32)

def to_slab(stored, count):
    width = stored.shape[1]
    return stored.reshape(count, ORDER // (count * NB), NB, width).transpose(1, 0, 2, 3).reshape(ORDER, width)

def to_stored(slab, count):
    width = slab.shape[1]
    return slab.reshape(ORDER // (count * NB), count, NB, width).transpose(1, 0, 2, 3).reshape(ORDER, width)

def reference(archive, slab_index, targets):
    descriptors = jnp.take(archive, slab_index, axis=0)
    positions = jnp.arange(ORDER, dtype=jnp.int32)
    right_side = to_slab(targets, N_COL)
    leading = PANELS * NB
    columns = matern(descriptors, descriptors[:leading], positions, positions[:leading])
    identity = jnp.eye(NB, dtype=jnp.float32)
    panel_list = []
    for step in range(PANELS):
        first = step * NB
        column = columns[:, first:first + NB]
        for earlier in panel_list:
            column = column - outer_product(earlier, earlier[first:first + NB])
        lower = jnp.linalg.cholesky(column[first:first + NB])
        inverse = lax.linalg.triangular_solve(lower, identity, left_side=True, lower=True)
        panel_list.append(outer_product(column, inverse))
    stacked = jnp.concatenate(panel_list, axis=1)

    def kernel_rows(rows):
        return product(matern(jnp.take(descriptors, rows, axis=0), descriptors, rows, positions), right_side)
    whole = lax.map(kernel_rows, positions.reshape(ORDER // NB, NB)).reshape(ORDER, NT)
    result = whole - product(stacked, product(stacked.T, right_side))
    return (to_stored(stacked, N_ROW), to_stored(result, N_ROW))
```

```python
import functools

import jax
import jax.numpy as jnp
from jax import lax
from jax.experimental import pallas as pl
from jax.experimental.pallas import tpu as pltpu
from jax.sharding import PartitionSpec as P

ORDER = 12288
F = 256
NB = 256
PANELS = 2
NT = 256
LEAD = PANELS * NB
SIDE = 16
LOCAL = ORDER // SIDE
PIECE = LOCAL // SIDE
LEAD_PIECE = LEAD // 8
TILES = LOCAL // NB
ROUND = 8
CHUNK = 128

precise = lax.Precision.HIGHEST
nugget = 1.0
scale = 5.0**0.5 / 16.0


def row_shift(value, dy, dz):
    pairs = [(y * 4 + z, (y + dy) % 4 * 4 + (z + dz) % 4) for y in range(4) for z in range(4)]
    return lax.ppermute(value, "row", pairs)


def col_shift(value, dh, dx, dk):
    pairs = [
        ((h * 4 + x) * 2 + k, ((h + dh) % 2 * 4 + (x + dx) % 4) * 2 + (k + dk) % 2)
        for h in range(2)
        for x in range(4)
        for k in range(2)
    ]
    return lax.ppermute(value, "col", pairs)


def flip(value):
    pairs = [(r * SIDE + c, c * SIDE + r) for r in range(SIDE) for c in range(SIDE)]
    return lax.ppermute(value, ("row", "col"), pairs)


def dot(left, right, left_dim, right_dim, precision=None):
    return lax.dot_general(
        left,
        right,
        (((left_dim,), (right_dim,)), ((), ())),
        precision=precision,
        preferred_element_type=jnp.float32,
    )


def split(value):
    high = value.astype(jnp.bfloat16)
    low = (value - high.astype(jnp.float32)).astype(jnp.bfloat16)
    return high, low


def dot3(left, right, left_dim, right_dim):
    left_high, left_low = left
    right_high, right_low = right
    small = dot(left_high, right_low, left_dim, right_dim) + dot(left_low, right_high, left_dim, right_dim)
    return small + dot(left_high, right_high, left_dim, right_dim)


def lane_squares(value):
    square = value * value
    ones = jnp.ones((8, square.shape[1]), jnp.float32)
    return dot(ones, square, 1, 1, precise)[0:1, :]


def matern(left_sq, right_sq, cross):
    clipped = jnp.maximum(left_sq + right_sq - 2.0 * cross, 1.0)
    scaled = clipped * lax.rsqrt(clipped) * scale
    return (1.0 + scaled + clipped * (scale * scale / 3.0)) * jnp.exp(-scaled)


def diagonal(shape, offset):
    left = lax.broadcasted_iota(jnp.int32, shape, 0) + offset
    return left == lax.broadcasted_iota(jnp.int32, shape, 1)


def eliminate(rows):
    lane = lax.broadcasted_iota(jnp.int32, (8, 128), 1)
    sub = lax.broadcasted_iota(jnp.int32, (8, 128), 0)
    pivots = [None] * 16

    def across(value, index):
        return jnp.broadcast_to(value[:, index : index + 1], (8, 128))

    def down(value, index):
        return jnp.broadcast_to(value[index : index + 1, :], (8, 128))

    for start in range(0, 128, ROUND):
        first = start // 8
        columns = [{v: across(rows[v], start + t) for v in range(first, 16)} for t in range(ROUND)]
        for t in range(ROUND):
            own, inner = (start + t) // 8, (start + t) % 8
            pivot = down(columns[t][own], inner)
            inverse = 1.0 / pivot
            pivots[own] = pivot if inner == 0 else jnp.where(sub >= inner, pivot, pivots[own])
            row = jnp.where(lane == start + t, 1.0 + pivot, down(rows[own], inner))
            later = [down(columns[u][own], inner) for u in range(t + 1, ROUND)]
            for v in range(own, 16):
                if v == own and inner == 7:
                    continue
                factor = columns[t][v] * inverse
                if v == own:
                    factor = jnp.where(sub > inner, factor, 0.0)
                rows[v] = rows[v] - factor * row
                for u in range(t + 1, ROUND):
                    columns[u][v] = columns[u][v] - factor * later[u - t - 1]
    result = []
    for v in range(16):
        unit = jnp.where(lane < sub + 8 * v, rows[v], jnp.where(lane == sub + 8 * v, 1.0, 0.0))
        result.append(unit * lax.rsqrt(pivots[v]))
    return jnp.concatenate(result, axis=0)


def gather_lead(x_place, own_ref, other_ref, k_place, lead_ref):
    for back in range(4):
        at = (x_place - back + 4) % 4 * 2
        lead_ref[pl.ds(pl.multiple_of((at + k_place) * LEAD_PIECE, 8), LEAD_PIECE), :] = own_ref[back]
        lead_ref[pl.ds(pl.multiple_of((at + 1 - k_place) * LEAD_PIECE, 8), LEAD_PIECE), :] = other_ref[back]


def factor_kernel(place_ref, own_ref, other_ref, lead_ref, out_ref):
    gather_lead(place_ref[0], own_ref, other_ref, place_ref[1], lead_ref)
    lead = lead_ref[...]
    left_sq = jnp.sum(lead * lead, axis=1, keepdims=True)
    block = matern(left_sq, lane_squares(lead), dot(lead, lead, 1, 1, precise))
    out_ref[...] = block + jnp.where(diagonal((LEAD, LEAD), 0), nugget, 0.0)
    wide = lax.broadcasted_iota(jnp.int32, (128, LEAD), 1)
    tall = lax.broadcasted_iota(jnp.int32, (LEAD, 128), 0)

    def step(index, carry):
        off = pl.multiple_of(index * 128, 128)
        here = pl.ds(off, 128)
        inverse = eliminate([out_ref[pl.ds(off + 8 * v, 8), here] for v in range(16)])
        below = jnp.where(tall >= off + 128, dot(out_ref[:, here], inverse, 1, 1, precise), 0.0)
        across = dot(inverse, out_ref[here, :], 1, 0, precise)
        out_ref[:, here] = jnp.where(tall >= off + 128, 0.0, out_ref[:, here])
        out_ref[here, :] = across
        out_ref[here, here] = inverse
        across = out_ref[here, :]
        out_ref[...] = out_ref[...] - dot(below, across, 1, 0, precise)
        out_ref[here, :] = jnp.where(wide < off + 128, across, 0.0)
        return carry

    lax.fori_loop(0, LEAD // 128, step, 0)


def slab_kernel(
    place_ref, own_rows, other_rows, col_pieces, lead_ref, inverse_ref, targets_ref,
    panel_ref, part_ref,
    rows_ref, cols_ref, cols_high, cols_low, goal_high, goal_low, lead_high, lead_low, inv_high, inv_low,
    gram_ref,
):
    y, z, h, x, k = (place_ref[i] for i in range(5))
    row_place, col_place = place_ref[5], place_ref[6]
    for back in range(4):
        for turn in range(2):
            at = ((h + turn) % 2 * 4 + (x - back + 4) % 4) * 2
            rows_ref[pl.ds(pl.multiple_of((at + k) * PIECE, 8), PIECE), :] = own_rows[back, turn]
            rows_ref[pl.ds(pl.multiple_of((at + 1 - k) * PIECE, 8), PIECE), :] = other_rows[back, turn]
    for z_back in range(4):
        for y_back in range(4):
            at = (y - y_back + 4) % 4 * 4 + (z - z_back + 4) % 4
            cols_ref[pl.ds(pl.multiple_of(at * PIECE, 8), PIECE), :] = col_pieces[z_back][y_back]
    cols_high[...], cols_low[...] = split(cols_ref[...])
    goal_high[...], goal_low[...] = split(targets_ref[...])
    lead_high[...], lead_low[...] = split(lead_ref[...])
    inv_high[...], inv_low[...] = split(inverse_ref[...])
    cols = (cols_high, cols_low)
    goal = (goal_high, goal_low)
    lead = (lead_high, lead_low)
    inv = (inv_high, inv_low)

    def whole(pair):
        return pair[0][...], pair[1][...]

    def at(pair, where):
        return pair[0][where, :], pair[1][where, :]

    lead_lane = lane_squares(lead_ref[...])
    col_lane = lane_squares(cols_ref[...])
    far = 1 << 20

    def lead_step(index, carry):
        where = pl.ds(pl.multiple_of(index * CHUNK, CHUNK), CHUNK)
        left = lead_ref[where, :]
        left_sq = jnp.sum(left * left, axis=1, keepdims=True)
        block = matern(left_sq, col_lane, dot3(at(lead, where), whole(cols), 1, 1))
        shift = index * CHUNK - col_place * NB
        block = block + jnp.where(
            diagonal((CHUNK, LOCAL), jnp.where((shift >= 0) & (shift < NB), shift, far)), nugget, 0.0
        )
        gram_ref[where, :] = dot3(split(block), whole(goal), 1, 0)
        return carry

    lax.fori_loop(0, LEAD // CHUNK, lead_step, 0)
    weights = split(dot3(whole(inv), split(gram_ref[...]), 1, 0))

    def row_step(index, carry):
        where = pl.ds(pl.multiple_of(index * CHUNK, CHUNK), CHUNK)
        left = rows_ref[where, :]
        left_sq = jnp.sum(left * left, axis=1, keepdims=True)
        pair = split(left)
        block = matern(left_sq, lead_lane, dot3(pair, whole(lead), 1, 1))
        inside = (index * CHUNK < NB) & (row_place < PANELS)
        shift = jnp.where(inside, index * CHUNK + row_place * NB, far)
        block = block + jnp.where(diagonal((CHUNK, LEAD), shift), nugget, 0.0)
        panel = dot3(split(block), whole(inv), 1, 1)
        panel_ref[where, :] = panel
        block = matern(left_sq, col_lane, dot3(pair, whole(cols), 1, 1))
        shift = jnp.where(row_place == col_place, index * CHUNK, far)
        block = block + jnp.where(diagonal((CHUNK, LOCAL), shift), nugget, 0.0)
        part_ref[where, :] = dot3(split(block), whole(goal), 1, 0) - dot3(split(panel), weights, 1, 0)
        return carry

    lax.fori_loop(0, LOCAL // CHUNK, row_step, 0)


def per_device(archive, slab_index, targets):
    row_place = lax.axis_index("row")
    col_place = lax.axis_index("col")
    y, z = row_place // 4, row_place % 4
    h, x, k = col_place // 8, col_place // 2 % 4, col_place % 2
    shard = archive.shape[0]

    def pick(ids):
        ids = ids - row_place * shard
        inside = (ids >= 0) & (ids < shard)
        picked = jnp.take(archive, jnp.clip(ids, 0, shard - 1), axis=0)
        return jnp.where(inside[..., None], picked, 0.0)

    lead_ids = lax.dynamic_slice_in_dim(slab_index, (x * 2 + k) * LEAD_PIECE, LEAD_PIECE, 0)
    lead = pick(lead_ids)
    lead = lead + row_shift(lead, 1, 0) + row_shift(lead, 2, 0) + row_shift(lead, 3, 0)
    lead = lead + row_shift(lead, 0, 1) + row_shift(lead, 0, 2) + row_shift(lead, 0, 3)
    lead_own = jnp.stack([lead] + [col_shift(lead, 0, s, 0) for s in (1, 2, 3)])
    lead_other = col_shift(lead_own, 0, 0, 1)

    stored = slab_index.reshape(TILES, SIDE, NB).transpose(1, 0, 2).reshape(SIDE, LOCAL)
    wanted = lax.dynamic_slice_in_dim(stored, col_place * PIECE, PIECE, 1).reshape(4, 4, PIECE)
    wanted = lax.dynamic_slice_in_dim(jnp.concatenate([wanted, wanted], 0), y, 4, 0)
    wanted = lax.dynamic_slice_in_dim(jnp.concatenate([wanted, wanted], 1), z, 4, 1)
    mine = pick(wanted[0])
    for s in (1, 2, 3):
        mine = mine + row_shift(pick(wanted[s]), s, 0)
    piece = mine[0]
    for s in (1, 2, 3):
        piece = piece + row_shift(mine[s], 0, s)

    pair = jnp.stack([piece, col_shift(piece, 1, 0, 0)])
    rows_own = jnp.stack([pair] + [col_shift(pair, 0, s, 0) for s in (1, 2, 3)])
    rows_other = col_shift(rows_own, 0, 0, 1)
    turned = flip(piece)
    turned = jnp.stack([turned] + [row_shift(turned, s, 0) for s in (1, 2, 3)])
    cols = [turned] + [row_shift(turned, 0, s) for s in (1, 2, 3)]

    place = jnp.stack([y, z, h, x, k, row_place, col_place]).astype(jnp.int32)
    smem = pl.BlockSpec(memory_space=pltpu.SMEM)
    vmem = pl.BlockSpec(memory_space=pltpu.VMEM)
    lead_all, inverse = pl.pallas_call(
        factor_kernel,
        out_shape=(
            jax.ShapeDtypeStruct((LEAD, F), jnp.float32),
            jax.ShapeDtypeStruct((LEAD, LEAD), jnp.float32),
        ),
        in_specs=[smem, vmem, vmem],
        out_specs=(vmem, vmem),
        name="factor",
    )(jnp.stack([x, k]).astype(jnp.int32), lead_own, lead_other)

    def slab_body(place_ref, own_rows, other_rows, c0, c1, c2, c3, *rest):
        slab_kernel(place_ref, own_rows, other_rows, (c0, c1, c2, c3), *rest)

    panels, part = pl.pallas_call(
        slab_body,
        out_shape=(
            jax.ShapeDtypeStruct((LOCAL, LEAD), jnp.float32),
            jax.ShapeDtypeStruct((LOCAL, NT), jnp.float32),
        ),
        in_specs=[smem] + [vmem] * 9,
        out_specs=(vmem, vmem),
        scratch_shapes=[
            pltpu.VMEM((LOCAL, F), jnp.float32),
            pltpu.VMEM((LOCAL, F), jnp.float32),
            pltpu.VMEM((LOCAL, F), jnp.bfloat16),
            pltpu.VMEM((LOCAL, F), jnp.bfloat16),
            pltpu.VMEM((LOCAL, NT), jnp.bfloat16),
            pltpu.VMEM((LOCAL, NT), jnp.bfloat16),
            pltpu.VMEM((LEAD, F), jnp.bfloat16),
            pltpu.VMEM((LEAD, F), jnp.bfloat16),
            pltpu.VMEM((LEAD, LEAD), jnp.bfloat16),
            pltpu.VMEM((LEAD, LEAD), jnp.bfloat16),
            pltpu.VMEM((LEAD, NT), jnp.float32),
        ],
        name="slab",
    )(place, rows_own, rows_other, *cols, lead_all, inverse, targets)

    part = part.reshape(2, 4, 2, PIECE, NT)
    keep = lax.dynamic_index_in_dim(part, k, 2, keepdims=False)
    send = lax.dynamic_index_in_dim(part, 1 - k, 2, keepdims=False)
    part = keep + col_shift(send, 0, 0, 1)
    total = lax.dynamic_index_in_dim(part, x, 1, keepdims=False)
    for s in (1, 2, 3):
        total = total + col_shift(lax.dynamic_index_in_dim(part, (x + s) % 4, 1, keepdims=False), 0, s, 0)
    result = lax.dynamic_index_in_dim(total, h, 0, keepdims=False)
    result = result + col_shift(lax.dynamic_index_in_dim(total, 1 - h, 0, keepdims=False), 1, 0, 0)
    return (panels, result)


def solution(mesh):
    placed = (P("row", None), P(), P("col", None))
    return jax.shard_map(
        per_device,
        mesh=mesh,
        in_specs=placed,
        out_specs=(P("row", None), P(("row", "col"), None)),
        check_vma=False,
    )
```

```python
import functools

import jax
import jax.numpy as jnp
from jax import lax
from jax.experimental import pallas as pl
from jax.experimental.pallas import tpu as pltpu
from jax.sharding import PartitionSpec as P


ORDER = 12288
F = 256
NB = 256
PANELS = 2
NT = 256
LEAD = PANELS * NB
SIDE = 16
LOCAL = ORDER // SIDE
PIECE = LOCAL // SIDE
LEAD_PIECE = LEAD // 8
TILES = LOCAL // NB
ROUND = 8

precise = lax.Precision.HIGHEST
nugget = 1.0
scale = 5.0**0.5 / 16.0


def row_swap(value, dy, dz):
    pairs = [(y * 4 + z, (y ^ dy) * 4 + (z ^ dz)) for y in range(4) for z in range(4)]
    return lax.ppermute(value, "row", pairs)


def col_swap(value, dh, dx, dk):
    pairs = [
        ((h * 4 + x) * 2 + k, ((h ^ dh) * 4 + (x ^ dx)) * 2 + (k ^ dk))
        for h in range(2)
        for x in range(4)
        for k in range(2)
    ]
    return lax.ppermute(value, "col", pairs)


def flip(value):
    pairs = [(r * SIDE + c, c * SIDE + r) for r in range(SIDE) for c in range(SIDE)]
    return lax.ppermute(value, ("row", "col"), pairs)


def dot(left, right, left_dim, right_dim, precision=None):
    return lax.dot_general(
        left,
        right,
        (((left_dim,), (right_dim,)), ((), ())),
        precision=precision,
        preferred_element_type=jnp.float32,
    )


def split(value):
    high = value.astype(jnp.bfloat16)
    low = (value - high.astype(jnp.float32)).astype(jnp.bfloat16)
    return high, low


def dot3(left, right, left_dim, right_dim):
    left_high, left_low = left
    right_high, right_low = right
    small = dot(left_high, right_low, left_dim, right_dim) + dot(left_low, right_high, left_dim, right_dim)
    return small + dot(left_high, right_high, left_dim, right_dim)


def lane_squares(value):
    square = value * value
    ones = jnp.ones((8, square.shape[1]), jnp.float32)
    return dot(ones, square, 1, 1, precise)[0:1, :]


def matern(left_sq, right_sq, cross):
    clipped = jnp.maximum(left_sq + right_sq + cross, scale * scale)
    scaled = clipped * lax.rsqrt(clipped)
    return (1.0 + scaled + clipped * (1.0 / 3.0)) * jnp.exp(-scaled)


def unit(shape, row_offset, lane_offset, bound):
    row = lax.broadcasted_iota(jnp.int32, shape, 0)
    lane = lax.broadcasted_iota(jnp.int32, shape, 1)
    return jnp.where((row + row_offset == lane + lane_offset) & (bound(row, lane) < NB), nugget, 0.0)


def eliminate(rows):
    lane = lax.broadcasted_iota(jnp.int32, (8, 128), 1)
    sub = lax.broadcasted_iota(jnp.int32, (8, 128), 0)
    pivots = [None] * 16

    def across(value, index):
        return jnp.broadcast_to(value[:, index : index + 1], (8, 128))

    def down(value, index):
        return jnp.broadcast_to(value[index : index + 1, :], (8, 128))

    for start in range(0, 128, ROUND):
        first = start // 8
        columns = [{v: across(rows[v], start + t) for v in range(first, 16)} for t in range(ROUND)]
        for t in range(ROUND):
            own, inner = (start + t) // 8, (start + t) % 8
            pivot = down(columns[t][own], inner)
            inverse = 1.0 / pivot
            pivots[own] = pivot if inner == 0 else jnp.where(sub >= inner, pivot, pivots[own])
            row = jnp.where(lane == start + t, 1.0 + pivot, down(rows[own], inner))
            later = [down(columns[u][own], inner) for u in range(t + 1, ROUND)]
            for v in range(own, 16):
                if v == own and inner == 7:
                    continue
                factor = columns[t][v] * inverse
                if v == own:
                    factor = jnp.where(sub > inner, factor, 0.0)
                rows[v] = rows[v] - factor * row
                for u in range(t + 1, ROUND):
                    columns[u][v] = columns[u][v] - factor * later[u - t - 1]
    result = []
    for v in range(16):
        unit = jnp.where(lane < sub + 8 * v, rows[v], jnp.where(lane == sub + 8 * v, 1.0, 0.0))
        result.append(unit * lax.rsqrt(pivots[v]))
    return jnp.concatenate(result, axis=0)


def aligned(start):
    return pl.multiple_of(start, 8)


def aligned(start):
    return pl.multiple_of(start, 8)


def whole(pair):
    return pair[0][...], pair[1][...]


def factor_block(off, in_ref, out_ref):
    here = slice(off, off + 128)
    inverse = eliminate([in_ref[off + 8 * v : off + 8 * v + 8, here] for v in range(16)])
    across = dot(inverse, in_ref[here, :], 1, 0, precise)
    if off:
        out_ref[:off, :] = in_ref[:off, :]
        out_ref[here, :off] = across[:, :off]
    out_ref[here, here] = inverse
    if off + 128 < LEAD:
        out_ref[here, off + 128 :] = jnp.zeros((128, LEAD - off - 128), jnp.float32)
        low = slice(off + 128, LEAD)
        below = dot(in_ref[low, here], inverse, 1, 1, precise)
        out_ref[low, low] = in_ref[low, low] - dot(below, across[:, off + 128 :], 1, 0, precise)
        if off:
            out_ref[low, :off] = in_ref[low, :off] - dot(below, across[:, :off], 1, 0, precise)
        out_ref[low, here] = -dot(below, inverse, 1, 0, precise)


def first_kernel(place_ref, own_ref, other_ref, lead_ref, out_ref, gram_ref):
    x, k = place_ref[3], place_ref[4]
    for s in range(4):
        at = (x ^ s) * 2
        lead_ref[pl.ds(aligned((at + k) * LEAD_PIECE), LEAD_PIECE), :] = own_ref[s] * scale
        lead_ref[pl.ds(aligned((at + 1 - k) * LEAD_PIECE), LEAD_PIECE), :] = other_ref[s] * scale
    lead = lead_ref[...]
    left_sq = jnp.sum(lead * lead, axis=1, keepdims=True)
    block = matern(left_sq, lane_squares(lead), dot(lead, lead * -2.0, 1, 1, precise))
    gram_ref[...] = block + unit((LEAD, LEAD), 0, 0, lambda row, lane: row * 0)
    factor_block(0, gram_ref, out_ref)


def slab_kernel(
    place_ref, own_rows, other_rows, c0, c1, c2, c3, lead_ref, inverse_ref, targets_ref,
    panel_ref, part_other_ref, part_own_ref,
    rows_ref, cols_ref, cols_high, cols_low, goal_high, goal_low, lead_high, lead_low, inv_high, inv_low,
):
    y, z, h, x, k, row_place, col_place = (place_ref[i] for i in range(7))
    for s in range(4):
        for e in range(2):
            at = ((h ^ e) * 4 + (x ^ s)) * 2
            rows_ref[pl.ds(aligned((at + k) * PIECE), PIECE), :] = own_rows[s, e] * scale
            rows_ref[pl.ds(aligned((at + 1 - k) * PIECE), PIECE), :] = other_rows[s, e] * scale
    for a, ref in enumerate((c0, c1, c2, c3)):
        for b in range(4):
            at = (y ^ a) * 4 + (z ^ b)
            cols_ref[pl.ds(aligned(at * PIECE), PIECE), :] = ref[b] * scale
    cols_high[...], cols_low[...] = split(cols_ref[...] * -2.0)
    goal_high[...], goal_low[...] = split(targets_ref[...])
    lead_high[...], lead_low[...] = split(lead_ref[...] * -2.0)
    inv_high[...], inv_low[...] = split(inverse_ref[...])
    cols, goal, inv = (cols_high, cols_low), (goal_high, goal_low), (inv_high, inv_low)
    lead_lane = lane_squares(lead_ref[...])
    col_lane = lane_squares(cols_ref[...])

    left = lead_ref[...]
    block = matern(jnp.sum(left * left, axis=1, keepdims=True), col_lane, dot3(split(left), whole(cols), 1, 1))
    block = block + unit((LEAD, LOCAL), 0, col_place * NB, lambda row, lane: lane)
    gram = dot3(split(block), whole(goal), 1, 0)
    weights = split(dot3(whole(inv), split(gram), 1, 0))

    left = rows_ref[...]
    lead = (lead_high, lead_low)
    block = matern(jnp.sum(left * left, axis=1, keepdims=True), lead_lane, dot3(split(left), whole(lead), 1, 1))
    block = block + unit((LOCAL, LEAD), row_place * NB, 0, lambda row, lane: row)
    panel_ref[...] = dot3(split(block), whole(inv), 1, 1)

    same = jnp.where(row_place == col_place, nugget, 0.0)
    for core, part_ref in ((1 - k, part_other_ref), (k, part_own_ref)):
        spots = []
        for s in range(4):
            for e in range(2):
                at = ((h ^ e) * 4 + (x ^ s)) * 2 + core
                spots.append(pl.ds(aligned(at * PIECE), PIECE))
        left = jnp.concatenate([rows_ref[p, :] for p in spots], axis=0)
        block = matern(jnp.sum(left * left, axis=1, keepdims=True), col_lane, dot3(split(left), whole(cols), 1, 1))
        panel = jnp.concatenate([panel_ref[p, :] for p in spots], axis=0)
        diag = jnp.concatenate([targets_ref[p, :] for p in spots], axis=0)
        total = dot3(split(block), whole(goal), 1, 0)
        total = total + diag * same - dot3(split(panel), weights, 1, 0)
        for s in range(4):
            for e in range(2):
                n = (s * 2 + e) * PIECE
                part_ref[s, e] = total[n : n + PIECE]


def per_device(archive, slab_index, targets):
    row_place = lax.axis_index("row")
    col_place = lax.axis_index("col")
    y, z = row_place // 4, row_place % 4
    h, x, k = col_place // 8, col_place // 2 % 4, col_place % 2
    shard = archive.shape[0]
    smem = pl.BlockSpec(memory_space=pltpu.SMEM)
    vmem = pl.BlockSpec(memory_space=pltpu.VMEM)
    f32, bf16 = jnp.float32, jnp.bfloat16

    def array(kind, *shape):
        return jax.ShapeDtypeStruct(shape, kind)

    def near(array):
        return pltpu.with_memory_space_constraint(array, pltpu.VMEM)

    def call(kernel, name, outs, scratch, place, *args):
        return pl.pallas_call(
            kernel,
            out_shape=tuple(s if far else pltpu.VMEM(s.shape, s.dtype) for s, far in outs),
            in_specs=([] if place is None else [smem]) + [vmem] * len(args),
            out_specs=tuple(vmem for _ in outs),
            scratch_shapes=[pltpu.VMEM(s.shape, s.dtype) for s in scratch],
            compiler_params=pltpu.CompilerParams(vmem_limit_bytes=(40 if name == "slab" else 16) << 20),
        )(*([] if place is None else [place]), *args)

    def three(shift):
        received = []
        for s in (1, 2, 3):
            received.append(shift(s))
        return received

    place = jnp.stack([y, z, h, x, k, row_place, col_place]).astype(jnp.int32)

    stored = slab_index.reshape(TILES, SIDE, NB).transpose(1, 0, 2).reshape(SIDE, LOCAL)
    wanted = lax.dynamic_slice_in_dim(stored, col_place * PIECE, PIECE, 1).reshape(2, 2, 2, 2, PIECE)
    for axis, bit in enumerate((y // 2, y % 2, z // 2, z % 2)):
        wanted = jnp.where(bit == 1, jnp.flip(wanted, axis), wanted)
    lead_ids = lax.dynamic_slice_in_dim(slab_index, (x * 2 + k) * LEAD_PIECE, LEAD_PIECE, 0)
    ids = jnp.concatenate([lead_ids, wanted.reshape(-1)]) - row_place * shard
    inside = (ids >= 0) & (ids < shard)
    picked = jnp.take(archive, jnp.clip(ids, 0, shard - 1), axis=0)
    picked = jnp.where(inside[:, None], picked, 0.0)

    early = picked[:LEAD_PIECE]
    lead = early + sum(three(lambda s: row_swap(early, s, 0)))
    lead_sum = lead
    lead = lead + sum(three(lambda s: row_swap(lead_sum, 0, s)))
    lead_own = jnp.stack([lead] + three(lambda s: col_swap(lead, 0, s, 0)))
    lead_other = col_swap(lead_own, 0, 0, 1)

    picked = picked[LEAD_PIECE:].reshape(4, 4, PIECE, F)
    mine = picked[0] + sum(three(lambda s: row_swap(picked[s], s, 0)))
    piece = mine[0] + sum(three(lambda s: row_swap(mine[s], 0, s)))

    pair = jnp.stack([piece, col_swap(piece, 1, 0, 0)])
    rows_own = jnp.stack([pair] + three(lambda s: col_swap(pair, 0, s, 0)))
    rows_other = col_swap(rows_own, 0, 0, 1)
    turned = flip(piece)
    quarter = jnp.stack([turned] + three(lambda s: row_swap(turned, 0, s)))
    cols = [quarter] + three(lambda s: row_swap(quarter, s, 0))

    lead_all, inverse = call(
        first_kernel, "factor0", ((array(f32, LEAD, F), False), (array(f32, LEAD, LEAD), False)), (array(f32, LEAD, LEAD),),
        place, near(lead_own), near(lead_other),
    )
    for index in (1, 2, 3):
        (inverse,) = call(
            functools.partial(factor_block, index * 128),
            f"factor{index}",
            ((array(f32, LEAD, LEAD), False),),
            (),
            None,
            near(inverse),
        )
    panels, part_other, part_own = call(
        slab_kernel,
        "slab",
        (
            (array(f32, LOCAL, LEAD), True),
            (array(f32, 4, 2, PIECE, NT), False),
            (array(f32, 4, 2, PIECE, NT), False),
        ),
        (array(f32, LOCAL, F), array(f32, LOCAL, F))
        + (array(bf16, LOCAL, F),) * 4
        + (array(bf16, LEAD, F),) * 2
        + (array(bf16, LEAD, LEAD),) * 2,
        place, near(rows_own), near(rows_other), *(near(c) for c in cols), near(lead_all), near(inverse), targets,
    )

    total = part_own + col_swap(part_other, 0, 0, 1)
    result = total[0] + sum(three(lambda s: col_swap(total[s], 0, s, 0)))
    result = result[0] + col_swap(result[1], 1, 0, 0)
    return (panels, result)


def solution(mesh):
    placed = (P("row", None), P(), P("col", None))
    return jax.shard_map(
        per_device,
        mesh=mesh,
        in_specs=placed,
        out_specs=(P("row", None), P(("row", "col"), None)),
        check_vma=False,
    )
```

```python
import functools

import jax
import jax.numpy as jnp
from jax import lax
from jax.experimental import pallas as pl
from jax.experimental.pallas import tpu as pltpu
from jax.sharding import PartitionSpec as P


ORDER = 12288
F = 256
NB = 256
PANELS = 2
NT = 256
LEAD = PANELS * NB
SIDE = 16
LOCAL = ORDER // SIDE
PIECE = LOCAL // SIDE
LEAD_PIECE = LEAD // 8
TILES = LOCAL // NB
HALF = LOCAL // 2
ROUND = 8

precise = lax.Precision.HIGHEST
nugget = 1.0
scale = 5.0**0.5 / 16.0


def row_swap(value, dy, dz):
    pairs = [(y * 4 + z, (y ^ dy) * 4 + (z ^ dz)) for y in range(4) for z in range(4)]
    return lax.ppermute(value, "row", pairs)


def col_swap(value, dh, dx, dk):
    pairs = [
        ((h * 4 + x) * 2 + k, ((h ^ dh) * 4 + (x ^ dx)) * 2 + (k ^ dk))
        for h in range(2)
        for x in range(4)
        for k in range(2)
    ]
    return lax.ppermute(value, "col", pairs)


def flip(value):
    pairs = [(r * SIDE + c, c * SIDE + r) for r in range(SIDE) for c in range(SIDE)]
    return lax.ppermute(value, ("row", "col"), pairs)


def dot(left, right, left_dim, right_dim, precision=None):
    return lax.dot_general(
        left,
        right,
        (((left_dim,), (right_dim,)), ((), ())),
        precision=precision,
        preferred_element_type=jnp.float32,
    )


def split(value):
    high = value.astype(jnp.bfloat16)
    low = (value - high.astype(jnp.float32)).astype(jnp.bfloat16)
    return high, low


def dot3(left, right, left_dim, right_dim):
    left_high, left_low = left
    right_high, right_low = right
    small = dot(left_high, right_low, left_dim, right_dim) + dot(left_low, right_high, left_dim, right_dim)
    return small + dot(left_high, right_high, left_dim, right_dim)


def lane_squares(value):
    square = value * value
    ones = jnp.ones((8, square.shape[1]), jnp.float32)
    return dot(ones, square, 1, 1, precise)[0:1, :]


def matern(left_sq, right_sq, cross):
    clipped = jnp.maximum(left_sq + right_sq + cross, scale * scale)
    scaled = clipped * lax.rsqrt(clipped)
    return (1.0 + scaled + clipped * (1.0 / 3.0)) * jnp.exp(-scaled)


def eliminate(rows):
    lane = lax.broadcasted_iota(jnp.int32, (8, 128), 1)
    sub = lax.broadcasted_iota(jnp.int32, (8, 128), 0)
    pivots = [None] * 16

    def across(value, index):
        return jnp.broadcast_to(value[:, index : index + 1], (8, 128))

    def down(value, index):
        return jnp.broadcast_to(value[index : index + 1, :], (8, 128))

    for start in range(0, 128, ROUND):
        first = start // 8
        columns = [{v: across(rows[v], start + t) for v in range(first, 16)} for t in range(ROUND)]
        for t in range(ROUND):
            own, inner = (start + t) // 8, (start + t) % 8
            pivot = down(columns[t][own], inner)
            inverse = 1.0 / pivot
            pivots[own] = pivot if inner == 0 else jnp.where(sub >= inner, pivot, pivots[own])
            row = jnp.where(lane == start + t, 1.0 + pivot, down(rows[own], inner))
            later = [down(columns[u][own], inner) for u in range(t + 1, ROUND)]
            for v in range(own, 16):
                if v == own and inner == 7:
                    continue
                factor = columns[t][v] * inverse
                if v == own:
                    factor = jnp.where(sub > inner, factor, 0.0)
                rows[v] = rows[v] - factor * row
                for u in range(t + 1, ROUND):
                    columns[u][v] = columns[u][v] - factor * later[u - t - 1]
    result = []
    for v in range(16):
        unit = jnp.where(lane < sub + 8 * v, rows[v], jnp.where(lane == sub + 8 * v, 1.0, 0.0))
        result.append(unit * lax.rsqrt(pivots[v]))
    return jnp.concatenate(result, axis=0)


def aligned(start):
    return pl.multiple_of(start, 8)


def aligned(start):
    return pl.multiple_of(start, 8)


def whole(pair):
    return pair[0][...], pair[1][...]


def gram_kernel(place_ref, own_ref, other_ref, lead_ref, out_ref):
    x, k = place_ref[3], place_ref[4]
    for s in range(4):
        at = (x ^ s) * 2
        lead_ref[pl.ds(aligned((at + k) * LEAD_PIECE), LEAD_PIECE), :] = own_ref[s] * scale
        lead_ref[pl.ds(aligned((at + 1 - k) * LEAD_PIECE), LEAD_PIECE), :] = other_ref[s] * scale
    lead = lead_ref[...]
    left_sq = jnp.sum(lead * lead, axis=1, keepdims=True)
    block = matern(left_sq, lane_squares(lead), dot(lead, lead * -2.0, 1, 1, precise))
    row = lax.broadcasted_iota(jnp.int32, (LEAD, LEAD), 0)
    lane = lax.broadcasted_iota(jnp.int32, (LEAD, LEAD), 1)
    out_ref[...] = block + jnp.where(row == lane, nugget, 0.0)


def factor_kernel(first, in_ref, out_ref):
    out_ref[...] = in_ref[...]
    tall = lax.broadcasted_iota(jnp.int32, (LEAD - first, 128), 0) + first
    wide = lax.broadcasted_iota(jnp.int32, (128, LEAD), 1)

    def step(index, carry):
        off = pl.multiple_of(index * 128, 128)
        here = pl.ds(off, 128)
        inverse = eliminate([out_ref[pl.ds(off + 8 * v, 8), here] for v in range(16)])
        later = tall >= off + 128
        below = jnp.where(later, dot(out_ref[first:, here], inverse, 1, 1, precise), 0.0)
        across = dot(inverse, out_ref[here, :], 1, 0, precise)
        out_ref[first:, here] = jnp.where(later, 0.0, out_ref[first:, here])
        out_ref[here, :] = across
        out_ref[here, here] = inverse
        across = out_ref[here, :]
        out_ref[first:, :] = out_ref[first:, :] - dot(below, across, 1, 0, precise)
        out_ref[here, :] = jnp.where(wide < off + 128, across, 0.0)
        return carry

    lax.fori_loop(first // 128, first // 128 + 2, step, 0)


def slab_kernel(
    place_ref, own_rows, other_rows, c0, c1, c2, c3, lead_ref, inverse_ref, targets_ref,
    panel_ref, part_other_ref, part_own_ref,
    left_ref, sum_ref, cols_ref, cols_high, cols_low, goal_high, goal_low, lead_high, lead_low, inv_high, inv_low,
):
    y, z, h, x, k, row_place, col_place = (place_ref[i] for i in range(7))
    for a, ref in enumerate((c0, c1, c2, c3)):
        for b in range(4):
            at = (y ^ a) * 4 + (z ^ b)
            cols_ref[pl.ds(aligned(at * PIECE), PIECE), :] = ref[b] * scale
    left_ref[:HALF] = other_rows[...].reshape(HALF, F) * scale
    left_ref[HALF:] = own_rows[...].reshape(HALF, F) * scale
    cols_high[...], cols_low[...] = split(cols_ref[...] * -2.0)
    goal_high[...], goal_low[...] = split(targets_ref[...])
    lead_high[...], lead_low[...] = split(lead_ref[...] * -2.0)
    inv_high[...], inv_low[...] = split(inverse_ref[...])
    cols, goal, inv, lead = (cols_high, cols_low), (goal_high, goal_low), (inv_high, inv_low), (lead_high, lead_low)
    lead_lane = lane_squares(lead_ref[...])
    col_lane = lane_squares(cols_ref[...])

    left = lead_ref[...]
    block = matern(jnp.sum(left * left, axis=1, keepdims=True), col_lane, dot3(split(left), whole(cols), 1, 1))
    gram = dot3(split(block), whole(goal), 1, 0)
    nuggets = [targets_ref[:NB, :] * jnp.where(col_place == p, nugget, 0.0) for p in range(PANELS)]
    gram = gram + jnp.concatenate(nuggets, axis=0)
    weights = split(dot3(whole(inv), split(gram), 1, 0))
    same = jnp.where(row_place == col_place, nugget, 0.0)

    def panel_step(side, carry):
        core = jnp.where(side == 0, 1 - k, k)
        where = pl.ds(aligned(side * HALF), HALF)
        starts = [
            aligned((((h ^ e) * 4 + (x ^ s)) * 2 + core) * PIECE) for s in range(4) for e in range(2)
        ]
        left = left_ref[where, :]
        left_sq = jnp.sum(left * left, axis=1, keepdims=True)
        pair = split(left)
        block = matern(left_sq, lead_lane, dot3(pair, whole(lead), 1, 1))
        row = jnp.concatenate([lax.broadcasted_iota(jnp.int32, (PIECE, 1), 0) + start for start in starts], axis=0)
        spot = jnp.where(row < NB, row + row_place * NB, LEAD)
        lane = lax.broadcasted_iota(jnp.int32, (HALF, LEAD), 1)
        block = block + jnp.where(spot == lane, nugget, 0.0)
        panel = dot3(split(block), whole(inv), 1, 1)
        for n, start in enumerate(starts):
            panel_ref[pl.ds(start, PIECE), :] = panel[n * PIECE : n * PIECE + PIECE]
        block = matern(left_sq, col_lane, dot3(pair, whole(cols), 1, 1))
        diag = jnp.concatenate([targets_ref[pl.ds(start, PIECE), :] for start in starts], axis=0)
        sum_ref[where, :] = dot3(split(block), whole(goal), 1, 0) + diag * same - dot3(split(panel), weights, 1, 0)
        return carry

    lax.fori_loop(0, 2, panel_step, 0)
    part_other_ref[...] = sum_ref[:HALF, :].reshape(4, 2, PIECE, NT)
    part_own_ref[...] = sum_ref[HALF:, :].reshape(4, 2, PIECE, NT)


def per_device(archive, slab_index, targets):
    row_place = lax.axis_index("row")
    col_place = lax.axis_index("col")
    y, z = row_place // 4, row_place % 4
    h, x, k = col_place // 8, col_place // 2 % 4, col_place % 2
    shard = archive.shape[0]
    smem = pl.BlockSpec(memory_space=pltpu.SMEM)
    vmem = pl.BlockSpec(memory_space=pltpu.VMEM)
    f32, bf16 = jnp.float32, jnp.bfloat16

    def array(kind, *shape):
        return jax.ShapeDtypeStruct(shape, kind)

    def near(array):
        return pltpu.with_memory_space_constraint(array, pltpu.VMEM)

    def call(kernel, name, outs, scratch, place, *args):
        return pl.pallas_call(
            kernel,
            out_shape=tuple(s if far else pltpu.VMEM(s.shape, s.dtype) for s, far in outs),
            in_specs=([] if place is None else [smem]) + [vmem] * len(args),
            out_specs=tuple(vmem for _ in outs),
            scratch_shapes=[pltpu.VMEM(s.shape, s.dtype) for s in scratch],
            compiler_params=pltpu.CompilerParams(vmem_limit_bytes=(40 if name == "slab" else 16) << 20),
        )(*([] if place is None else [place]), *args)

    def three(shift):
        received = []
        for s in (1, 2, 3):
            received.append(shift(s))
        return received

    place = jnp.stack([y, z, h, x, k, row_place, col_place]).astype(jnp.int32)

    stored = slab_index.reshape(TILES, SIDE, NB).transpose(1, 0, 2).reshape(SIDE, LOCAL)
    wanted = lax.dynamic_slice_in_dim(stored, col_place * PIECE, PIECE, 1).reshape(2, 2, 2, 2, PIECE)
    for axis, bit in enumerate((y // 2, y % 2, z // 2, z % 2)):
        wanted = jnp.where(bit == 1, jnp.flip(wanted, axis), wanted)
    lead_ids = lax.dynamic_slice_in_dim(stored[:PANELS, :NB].reshape(-1), (x * 2 + k) * LEAD_PIECE, LEAD_PIECE, 0)
    ids = jnp.concatenate([lead_ids, wanted.reshape(-1)]) - row_place * shard
    inside = (ids >= 0) & (ids < shard)
    picked = jnp.take(archive, jnp.clip(ids, 0, shard - 1), axis=0)
    picked = jnp.where(inside[:, None], picked, 0.0)

    early = picked[:LEAD_PIECE]
    lead = early + sum(three(lambda s: row_swap(early, s, 0)))
    lead_sum = lead
    lead = lead + sum(three(lambda s: row_swap(lead_sum, 0, s)))
    lead_own = jnp.stack([lead] + three(lambda s: col_swap(lead, 0, s, 0)))
    lead_other = col_swap(lead_own, 0, 0, 1)

    picked = picked[LEAD_PIECE:].reshape(4, 4, PIECE, F)
    mine = picked[0] + sum(three(lambda s: row_swap(picked[s], s, 0)))
    piece = mine[0] + sum(three(lambda s: row_swap(mine[s], 0, s)))

    pair = jnp.stack([piece, col_swap(piece, 1, 0, 0)])
    rows_own = jnp.stack([pair] + three(lambda s: col_swap(pair, 0, s, 0)))
    rows_other = col_swap(rows_own, 0, 0, 1)
    turned = flip(piece)
    quarter = jnp.stack([turned] + three(lambda s: row_swap(turned, 0, s)))
    cols = [quarter] + three(lambda s: row_swap(quarter, s, 0))

    square = (array(f32, LEAD, LEAD), False)
    lead_all, inverse = call(
        gram_kernel, "gram", ((array(f32, LEAD, F), False), square), (), place, near(lead_own), near(lead_other)
    )
    for first in (0, LEAD // 2):
        (inverse,) = call(
            functools.partial(factor_kernel, first), f"factor{first}", (square,), (), None, near(inverse)
        )
    panels, part_other, part_own = call(
        slab_kernel,
        "slab",
        (
            (array(f32, LOCAL, LEAD), True),
            (array(f32, 4, 2, PIECE, NT), False),
            (array(f32, 4, 2, PIECE, NT), False),
        ),
        (array(f32, LOCAL, F), array(f32, LOCAL, NT), array(f32, LOCAL, F))
        + (array(bf16, LOCAL, F),) * 4
        + (array(bf16, LEAD, F),) * 2
        + (array(bf16, LEAD, LEAD),) * 2,
        place, near(rows_own), near(rows_other), *(near(c) for c in cols), near(lead_all), near(inverse), targets,
    )

    total = part_own + col_swap(part_other, 0, 0, 1)
    result = total[0] + sum(three(lambda s: col_swap(total[s], 0, s, 0)))
    result = result[0] + col_swap(result[1], 1, 0, 0)
    return (panels, result)


def solution(mesh):
    placed = (P("row", None), P(), P("col", None))
    return jax.shard_map(
        per_device,
        mesh=mesh,
        in_specs=placed,
        out_specs=(P("row", None), P(("row", "col"), None)),
        check_vma=False,
    )
```

```python
import functools

import jax
import jax.numpy as jnp
from jax import lax
from jax.experimental import pallas as pl
from jax.experimental.pallas import tpu as pltpu
from jax.sharding import PartitionSpec as P


ORDER = 12288
F = 256
NB = 256
PANELS = 2
NT = 256
LEAD = PANELS * NB
SIDE = 16
LOCAL = ORDER // SIDE
PIECE = LOCAL // SIDE
LEAD_PIECE = LEAD // 8
TILES = LOCAL // NB
HALF = LOCAL // 2
ROUND = 8

nugget = 1.0
scale = 5.0**0.5 / 16.0


def row_swap(value, dy, dz):
    pairs = [(y * 4 + z, (y ^ dy) * 4 + (z ^ dz)) for y in range(4) for z in range(4)]
    return lax.ppermute(value, "row", pairs)


def col_swap(value, dh, dx, dk):
    pairs = [
        ((h * 4 + x) * 2 + k, ((h ^ dh) * 4 + (x ^ dx)) * 2 + (k ^ dk))
        for h in range(2)
        for x in range(4)
        for k in range(2)
    ]
    return lax.ppermute(value, "col", pairs)


def flip(value):
    pairs = [(r * SIDE + c, c * SIDE + r) for r in range(SIDE) for c in range(SIDE)]
    return lax.ppermute(value, ("row", "col"), pairs)


def dot(left, right, left_dim, right_dim):
    return lax.dot_general(
        left,
        right,
        (((left_dim,), (right_dim,)), ((), ())),
        preferred_element_type=jnp.float32,
    )


def split(value):
    high = value.astype(jnp.bfloat16)
    low = (value - high.astype(jnp.float32)).astype(jnp.bfloat16)
    return high, low


def dot3(left, right, left_dim, right_dim):
    left_high, left_low = left
    right_high, right_low = right
    small = dot(left_high, right_low, left_dim, right_dim) + dot(left_low, right_high, left_dim, right_dim)
    return small + dot(left_high, right_high, left_dim, right_dim)


def lane_squares(value):
    rest, total = value * value, 0.0
    ones = jnp.ones((16, value.shape[1]), jnp.bfloat16)
    for _ in range(3):
        term = rest.astype(jnp.bfloat16)
        rest = rest - term.astype(jnp.float32)
        total = total + dot(ones, term, 1, 1)
    return total[0:1, :]


def matern(left_sq, right_sq, cross):
    clipped = jnp.maximum(left_sq + right_sq + cross, scale * scale)
    scaled = clipped * lax.rsqrt(clipped)
    return (1.0 + scaled + clipped * (1.0 / 3.0)) * jnp.exp(-scaled)


def eliminate(rows):
    lane = lax.broadcasted_iota(jnp.int32, (8, 128), 1)
    sub = lax.broadcasted_iota(jnp.int32, (8, 128), 0)
    pivots = [None] * 16

    def across(value, index):
        return jnp.broadcast_to(value[:, index : index + 1], (8, 128))

    def down(value, index):
        return jnp.broadcast_to(value[index : index + 1, :], (8, 128))

    for start in range(0, 128, ROUND):
        first = start // 8
        columns = [{v: across(rows[v], start + t) for v in range(first, 16)} for t in range(ROUND)]
        for t in range(ROUND):
            own, inner = (start + t) // 8, (start + t) % 8
            pivot = down(columns[t][own], inner)
            inverse = 1.0 / pivot
            pivots[own] = pivot if inner == 0 else jnp.where(sub >= inner, pivot, pivots[own])
            row = jnp.where(lane == start + t, 1.0 + pivot, down(rows[own], inner))
            later = [down(columns[u][own], inner) for u in range(t + 1, ROUND)]
            for v in range(own, 16):
                if v == own and inner == 7:
                    continue
                factor = columns[t][v] * inverse
                if v == own:
                    factor = jnp.where(sub > inner, factor, 0.0)
                rows[v] = rows[v] - factor * row
                for u in range(t + 1, ROUND):
                    columns[u][v] = columns[u][v] - factor * later[u - t - 1]
    result = []
    for v in range(16):
        unit = jnp.where(lane < sub + 8 * v, rows[v], jnp.where(lane == sub + 8 * v, 1.0, 0.0))
        result.append(unit * lax.rsqrt(pivots[v]))
    return jnp.concatenate(result, axis=0)


def aligned(start):
    return pl.multiple_of(start, 8)


def aligned(start):
    return pl.multiple_of(start, 8)


def whole(pair):
    return pair[0][...], pair[1][...]


def gram_kernel(place_ref, own_ref, other_ref, lead_ref, out_ref):
    x, k = place_ref[3], place_ref[4]
    for s in range(4):
        at = (x ^ s) * 2
        lead_ref[pl.ds(aligned((at + k) * LEAD_PIECE), LEAD_PIECE), :] = own_ref[s] * scale
        lead_ref[pl.ds(aligned((at + 1 - k) * LEAD_PIECE), LEAD_PIECE), :] = other_ref[s] * scale
    lead = lead_ref[...]
    left_sq = jnp.sum(lead * lead, axis=1, keepdims=True)
    block = matern(left_sq, lane_squares(lead), dot3(split(lead), split(lead * -2.0), 1, 1))
    row = lax.broadcasted_iota(jnp.int32, (LEAD, LEAD), 0)
    lane = lax.broadcasted_iota(jnp.int32, (LEAD, LEAD), 1)
    out_ref[...] = block + jnp.where(row == lane, nugget, 0.0)


def factor_kernel(first, in_ref, out_ref):
    out_ref[...] = in_ref[...]
    tall = lax.broadcasted_iota(jnp.int32, (LEAD - first, 128), 0) + first
    wide = lax.broadcasted_iota(jnp.int32, (128, LEAD), 1)

    def step(index, carry):
        off = pl.multiple_of(index * 128, 128)
        here = pl.ds(off, 128)
        inverse = eliminate([out_ref[pl.ds(off + 8 * v, 8), here] for v in range(16)])
        later = tall >= off + 128
        pair = split(inverse)
        below = jnp.where(later, dot3(split(out_ref[first:, here]), pair, 1, 1), 0.0)
        across = dot3(pair, split(out_ref[here, :]), 1, 0)
        out_ref[first:, here] = jnp.where(later, 0.0, out_ref[first:, here])
        out_ref[here, :] = across
        out_ref[here, here] = inverse
        across = out_ref[here, :]
        out_ref[first:, :] = out_ref[first:, :] - dot3(split(below), split(across), 1, 0)
        out_ref[here, :] = jnp.where(wide < off + 128, across, 0.0)
        return carry

    lax.fori_loop(first // 128, first // 128 + 2, step, 0)


def slab_kernel(
    place_ref, own_rows, other_rows, c0, c1, c2, c3, lead_ref, inverse_ref, targets_ref,
    panel_ref, part_other_ref, part_own_ref,
    left_ref, cols_ref, cols_high, cols_low, goal_high, goal_low, lead_high, lead_low, inv_high, inv_low,
):
    y, z, h, x, k, row_place, col_place = (place_ref[i] for i in range(7))
    for a, ref in enumerate((c0, c1, c2, c3)):
        for b in range(4):
            at = (y ^ a) * 4 + (z ^ b)
            cols_ref[pl.ds(aligned(at * PIECE), PIECE), :] = ref[b] * scale
    left_ref[:HALF] = other_rows[...].reshape(HALF, F) * scale
    left_ref[HALF:] = own_rows[...].reshape(HALF, F) * scale
    cols_high[...], cols_low[...] = split(cols_ref[...] * -2.0)
    goal_high[...], goal_low[...] = split(targets_ref[...])
    lead_high[...], lead_low[...] = split(lead_ref[...] * -2.0)
    inv_high[...], inv_low[...] = split(inverse_ref[...])
    cols, goal, inv, lead = (cols_high, cols_low), (goal_high, goal_low), (inv_high, inv_low), (lead_high, lead_low)
    lead_lane = lane_squares(lead_ref[...])
    col_lane = lane_squares(cols_ref[...])

    left = lead_ref[...]
    block = matern(jnp.sum(left * left, axis=1, keepdims=True), col_lane, dot3(split(left), whole(cols), 1, 1))
    gram = dot3(split(block), whole(goal), 1, 0)
    nuggets = [targets_ref[:NB, :] * jnp.where(col_place == p, nugget, 0.0) for p in range(PANELS)]
    gram = gram + jnp.concatenate(nuggets, axis=0)
    weights = split(dot3(whole(inv), split(gram), 1, 0))
    same = jnp.where(row_place == col_place, nugget, 0.0)

    def starts_of(core):
        return [aligned((((h ^ e) * 4 + (x ^ s)) * 2 + core) * PIECE) for s in range(4) for e in range(2)]

    def panel_step(side, carry):
        starts = starts_of(jnp.where(side == 0, 1 - k, k))
        left = left_ref[pl.ds(aligned(side * HALF), HALF), :]
        left_sq = jnp.sum(left * left, axis=1, keepdims=True)
        block = matern(left_sq, lead_lane, dot3(split(left), whole(lead), 1, 1))
        row = jnp.concatenate([lax.broadcasted_iota(jnp.int32, (PIECE, 1), 0) + start for start in starts], axis=0)
        spot = jnp.where(row < NB, row + row_place * NB, LEAD)
        lane = lax.broadcasted_iota(jnp.int32, (HALF, LEAD), 1)
        block = block + jnp.where(spot == lane, nugget, 0.0)
        panel = dot3(split(block), whole(inv), 1, 1)
        for n, start in enumerate(starts):
            panel_ref[pl.ds(start, PIECE), :] = panel[n * PIECE : n * PIECE + PIECE]
        return carry

    lax.fori_loop(0, 2, panel_step, 0)

    for side, part_ref in enumerate((part_other_ref, part_own_ref)):
        starts = starts_of((1 - k, k)[side])
        left = left_ref[side * HALF : side * HALF + HALF, :]
        left_sq = jnp.sum(left * left, axis=1, keepdims=True)
        block = matern(left_sq, col_lane, dot3(split(left), whole(cols), 1, 1))
        panel = jnp.concatenate([panel_ref[pl.ds(start, PIECE), :] for start in starts], axis=0)
        diag = jnp.concatenate([targets_ref[pl.ds(start, PIECE), :] for start in starts], axis=0)
        total = dot3(split(block), whole(goal), 1, 0) + diag * same - dot3(split(panel), weights, 1, 0)
        part_ref[...] = total.reshape(4, 2, PIECE, NT)


def per_device(archive, slab_index, targets):
    row_place = lax.axis_index("row")
    col_place = lax.axis_index("col")
    y, z = row_place // 4, row_place % 4
    h, x, k = col_place // 8, col_place // 2 % 4, col_place % 2
    shard = archive.shape[0]
    smem = pl.BlockSpec(memory_space=pltpu.SMEM)
    vmem = pl.BlockSpec(memory_space=pltpu.VMEM)
    f32, bf16 = jnp.float32, jnp.bfloat16

    def array(kind, *shape):
        return jax.ShapeDtypeStruct(shape, kind)

    def near(array):
        return pltpu.with_memory_space_constraint(array, pltpu.VMEM)

    def call(kernel, name, outs, scratch, place, *args):
        return pl.pallas_call(
            kernel,
            out_shape=tuple(s if far else pltpu.VMEM(s.shape, s.dtype) for s, far in outs),
            in_specs=([] if place is None else [smem]) + [vmem] * len(args),
            out_specs=tuple(vmem for _ in outs),
            scratch_shapes=[pltpu.VMEM(s.shape, s.dtype) for s in scratch],
            compiler_params=pltpu.CompilerParams(vmem_limit_bytes=(40 if name == "slab" else 16) << 20),
        )(*([] if place is None else [place]), *args)

    def three(shift):
        received = []
        for s in (1, 2, 3):
            received.append(shift(s))
        return received

    place = jnp.stack([y, z, h, x, k, row_place, col_place]).astype(jnp.int32)

    stored = slab_index.reshape(TILES, SIDE, NB).transpose(1, 0, 2).reshape(SIDE, LOCAL)
    wanted = lax.dynamic_slice_in_dim(stored, col_place * PIECE, PIECE, 1).reshape(2, 2, 2, 2, PIECE)
    for axis, bit in enumerate((y // 2, y % 2, z // 2, z % 2)):
        wanted = jnp.where(bit == 1, jnp.flip(wanted, axis), wanted)
    lead_ids = lax.dynamic_slice_in_dim(stored[:PANELS, :NB].reshape(-1), (x * 2 + k) * LEAD_PIECE, LEAD_PIECE, 0)
    ids = jnp.concatenate([lead_ids, wanted.reshape(-1)]) - row_place * shard
    inside = (ids >= 0) & (ids < shard)
    picked = jnp.take(archive, jnp.clip(ids, 0, shard - 1), axis=0)
    picked = jnp.where(inside[:, None], picked, 0.0)

    early = picked[:LEAD_PIECE]
    lead = early + sum(three(lambda s: row_swap(early, s, 0)))
    lead_sum = lead
    lead = lead + sum(three(lambda s: row_swap(lead_sum, 0, s)))
    lead_own = jnp.stack([lead] + three(lambda s: col_swap(lead, 0, s, 0)))
    lead_other = col_swap(lead_own, 0, 0, 1)

    picked = picked[LEAD_PIECE:].reshape(4, 4, PIECE, F)
    mine = picked[0] + sum(three(lambda s: row_swap(picked[s], s, 0)))
    piece = mine[0] + sum(three(lambda s: row_swap(mine[s], 0, s)))

    pair = jnp.stack([piece, col_swap(piece, 1, 0, 0)])
    rows_own = jnp.stack([pair] + three(lambda s: col_swap(pair, 0, s, 0)))
    rows_other = col_swap(rows_own, 0, 0, 1)
    turned = flip(piece)
    quarter = jnp.stack([turned] + three(lambda s: row_swap(turned, 0, s)))
    cols = [quarter] + three(lambda s: row_swap(quarter, s, 0))

    square = (array(f32, LEAD, LEAD), False)
    lead_all, inverse = call(
        gram_kernel, "gram", ((array(f32, LEAD, F), False), square), (), place, near(lead_own), near(lead_other)
    )
    for first in (0, LEAD // 2):
        (inverse,) = call(
            functools.partial(factor_kernel, first), f"factor{first}", (square,), (), None, near(inverse)
        )
    panels, part_other, part_own = call(
        slab_kernel,
        "slab",
        (
            (array(f32, LOCAL, LEAD), True),
            (array(f32, 4, 2, PIECE, NT), False),
            (array(f32, 4, 2, PIECE, NT), False),
        ),
        (array(f32, LOCAL, F), array(f32, LOCAL, F))
        + (array(bf16, LOCAL, F),) * 4
        + (array(bf16, LEAD, F),) * 2
        + (array(bf16, LEAD, LEAD),) * 2,
        place, near(rows_own), near(rows_other), *(near(c) for c in cols), near(lead_all), near(inverse), targets,
    )

    total = part_own + col_swap(part_other, 0, 0, 1)
    result = total[0] + sum(three(lambda s: col_swap(total[s], 0, s, 0)))
    result = result[0] + col_swap(result[1], 1, 0, 0)
    return (panels, result)


def solution(mesh):
    placed = (P("row", None), P(), P("col", None))
    return jax.shard_map(
        per_device,
        mesh=mesh,
        in_specs=placed,
        out_specs=(P("row", None), P(("row", "col"), None)),
        check_vma=False,
    )
```

```python
import functools

import jax
import jax.numpy as jnp
from jax import lax
from jax.experimental import pallas as pl
from jax.experimental.pallas import tpu as pltpu
from jax.sharding import PartitionSpec as P


ORDER = 12288
F = 256
NB = 256
PANELS = 2
NT = 256
LEAD = PANELS * NB
SIDE = 16
LOCAL = ORDER // SIDE
PIECE = LOCAL // SIDE
LEAD_PIECE = LEAD // 8
TILES = LOCAL // NB
HALF = LOCAL // 2
ROUND = 8

nugget = 1.0
scale = 5.0**0.5 / 16.0


def row_swap(value, dy, dz):
    pairs = [(y * 4 + z, (y ^ dy) * 4 + (z ^ dz)) for y in range(4) for z in range(4)]
    return lax.ppermute(value, "row", pairs)


def col_swap(value, dh, dx, dk):
    pairs = [
        ((h * 4 + x) * 2 + k, ((h ^ dh) * 4 + (x ^ dx)) * 2 + (k ^ dk))
        for h in range(2)
        for x in range(4)
        for k in range(2)
    ]
    return lax.ppermute(value, "col", pairs)


def flip(value):
    pairs = [(r * SIDE + c, c * SIDE + r) for r in range(SIDE) for c in range(SIDE)]
    return lax.ppermute(value, ("row", "col"), pairs)


def dot(left, right, left_dim, right_dim):
    return lax.dot_general(
        left,
        right,
        (((left_dim,), (right_dim,)), ((), ())),
        preferred_element_type=jnp.float32,
    )


def split(value):
    high = value.astype(jnp.bfloat16)
    low = (value - high.astype(jnp.float32)).astype(jnp.bfloat16)
    return high, low


def dot3(left, right, left_dim, right_dim):
    left_high, left_low = left
    right_high, right_low = right
    small = dot(left_high, right_low, left_dim, right_dim) + dot(left_low, right_high, left_dim, right_dim)
    return small + dot(left_high, right_high, left_dim, right_dim)


def lane_squares(value):
    rest, total = value * value, 0.0
    ones = jnp.ones((16, value.shape[1]), jnp.bfloat16)
    for _ in range(3):
        term = rest.astype(jnp.bfloat16)
        rest = rest - term.astype(jnp.float32)
        total = total + dot(ones, term, 1, 1)
    return total[0:1, :]


def matern(left_sq, right_sq, cross):
    clipped = jnp.maximum(left_sq + right_sq + cross, scale * scale)
    scaled = clipped * lax.rsqrt(clipped)
    return (1.0 + scaled + clipped * (1.0 / 3.0)) * jnp.exp(-scaled)


def eliminate(rows):
    lane = lax.broadcasted_iota(jnp.int32, (8, 128), 1)
    sub = lax.broadcasted_iota(jnp.int32, (8, 128), 0)
    pivots = [None] * 16

    def across(value, index):
        return jnp.broadcast_to(value[:, index : index + 1], (8, 128))

    def down(value, index):
        return jnp.broadcast_to(value[index : index + 1, :], (8, 128))

    for start in range(0, 128, ROUND):
        first = start // 8
        columns = [{v: across(rows[v], start + t) for v in range(first, 16)} for t in range(ROUND)]
        for t in range(ROUND):
            own, inner = (start + t) // 8, (start + t) % 8
            pivot = down(columns[t][own], inner)
            inverse = 1.0 / pivot
            pivots[own] = pivot if inner == 0 else jnp.where(sub >= inner, pivot, pivots[own])
            row = jnp.where(lane == start + t, 1.0 + pivot, down(rows[own], inner))
            later = [down(columns[u][own], inner) for u in range(t + 1, ROUND)]
            for v in range(own, 16):
                if v == own and inner == 7:
                    continue
                factor = columns[t][v] * inverse
                if v == own:
                    factor = jnp.where(sub > inner, factor, 0.0)
                rows[v] = rows[v] - factor * row
                for u in range(t + 1, ROUND):
                    columns[u][v] = columns[u][v] - factor * later[u - t - 1]
    result = []
    for v in range(16):
        unit = jnp.where(lane < sub + 8 * v, rows[v], jnp.where(lane == sub + 8 * v, 1.0, 0.0))
        result.append(unit * lax.rsqrt(pivots[v]))
    return jnp.concatenate(result, axis=0)


def aligned(start):
    return pl.multiple_of(start, 8)


def aligned(start):
    return pl.multiple_of(start, 8)


def whole(pair):
    return pair[0][...], pair[1][...]


def gram_kernel(place_ref, own_ref, other_ref, lead_ref, out_ref):
    x, k = place_ref[3], place_ref[4]
    for s in range(4):
        at = (x ^ s) * 2
        lead_ref[pl.ds(aligned((at + k) * LEAD_PIECE), LEAD_PIECE), :] = own_ref[s] * scale
        lead_ref[pl.ds(aligned((at + 1 - k) * LEAD_PIECE), LEAD_PIECE), :] = other_ref[s] * scale
    lead = lead_ref[...]
    left_sq = jnp.sum(lead * lead, axis=1, keepdims=True)
    block = matern(left_sq, lane_squares(lead), dot3(split(lead), split(lead * -2.0), 1, 1))
    row = lax.broadcasted_iota(jnp.int32, (LEAD, LEAD), 0)
    lane = lax.broadcasted_iota(jnp.int32, (LEAD, LEAD), 1)
    out_ref[...] = block + jnp.where(row == lane, nugget, 0.0)


def factor_kernel(first, in_ref, out_ref):
    out_ref[...] = in_ref[...]
    tall = lax.broadcasted_iota(jnp.int32, (LEAD - first, 128), 0) + first
    wide = lax.broadcasted_iota(jnp.int32, (128, LEAD), 1)

    def step(index, carry):
        off = pl.multiple_of(index * 128, 128)
        here = pl.ds(off, 128)
        inverse = eliminate([out_ref[pl.ds(off + 8 * v, 8), here] for v in range(16)])
        later = tall >= off + 128
        pair = split(inverse)
        below = jnp.where(later, dot3(split(out_ref[first:, here]), pair, 1, 1), 0.0)
        across = dot3(pair, split(out_ref[here, :]), 1, 0)
        out_ref[first:, here] = jnp.where(later, 0.0, out_ref[first:, here])
        out_ref[here, :] = across
        out_ref[here, here] = inverse
        across = out_ref[here, :]
        out_ref[first:, :] = out_ref[first:, :] - dot3(split(below), split(across), 1, 0)
        out_ref[here, :] = jnp.where(wide < off + 128, across, 0.0)
        return carry

    lax.fori_loop(first // 128, first // 128 + 2, step, 0)


def slab_kernel(
    place_ref, own_rows, other_rows, c0, c1, c2, c3, lead_ref, inverse_ref, targets_ref,
    panel_ref, part_other_ref, part_own_ref,
    left_ref, cols_ref, cols_high, cols_low, goal_high, goal_low, lead_high, lead_low, inv_high, inv_low,
):
    y, z, h, x, k, row_place, col_place = (place_ref[i] for i in range(7))
    for a, ref in enumerate((c0, c1, c2, c3)):
        for b in range(4):
            at = (y ^ a) * 4 + (z ^ b)
            cols_ref[pl.ds(aligned(at * PIECE), PIECE), :] = ref[b] * scale
    left_ref[:HALF] = other_rows[...].reshape(HALF, F) * scale
    left_ref[HALF:] = own_rows[...].reshape(HALF, F) * scale
    cols_high[...], cols_low[...] = split(cols_ref[...] * -2.0)
    goal_high[...], goal_low[...] = split(targets_ref[...])
    lead_high[...], lead_low[...] = split(lead_ref[...] * -2.0)
    inv_high[...], inv_low[...] = split(inverse_ref[...])
    cols, goal, lead = (cols_high, cols_low), (goal_high, goal_low), (lead_high, lead_low)
    lead_lane = lane_squares(lead_ref[...])
    col_lane = lane_squares(cols_ref[...])

    left = lead_ref[...]
    block = matern(jnp.sum(left * left, axis=1, keepdims=True), col_lane, dot3(split(left), whole(cols), 1, 1))
    gram = dot3(split(block), whole(goal), 1, 0)
    nuggets = [targets_ref[:NB, :] * jnp.where(col_place == p, nugget, 0.0) for p in range(PANELS)]
    gram = gram + jnp.concatenate(nuggets, axis=0)
    upper = (inv_high[:NB, :NB], inv_low[:NB, :NB])
    lower = (inv_high[NB:, :], inv_low[NB:, :])
    gram_high, gram_low = split(gram)
    weights = split(
        jnp.concatenate(
            [dot3(upper, (gram_high[:NB], gram_low[:NB]), 1, 0), dot3(lower, (gram_high, gram_low), 1, 0)], axis=0
        )
    )
    same = jnp.where(row_place == col_place, nugget, 0.0)

    def starts_of(core):
        return [aligned((((h ^ e) * 4 + (x ^ s)) * 2 + core) * PIECE) for s in range(4) for e in range(2)]

    def panel_step(side, carry):
        starts = starts_of(jnp.where(side == 0, 1 - k, k))
        left = left_ref[pl.ds(aligned(side * HALF), HALF), :]
        left_sq = jnp.sum(left * left, axis=1, keepdims=True)
        block = matern(left_sq, lead_lane, dot3(split(left), whole(lead), 1, 1))
        row = jnp.concatenate([lax.broadcasted_iota(jnp.int32, (PIECE, 1), 0) + start for start in starts], axis=0)
        spot = jnp.where(row < NB, row + row_place * NB, LEAD)
        lane = lax.broadcasted_iota(jnp.int32, (HALF, LEAD), 1)
        block = block + jnp.where(spot == lane, nugget, 0.0)
        high, low = split(block)
        panel = jnp.concatenate(
            [
                dot3((high[:, :NB], low[:, :NB]), (inv_high[:NB, :NB], inv_low[:NB, :NB]), 1, 1),
                dot3((high, low), (inv_high[NB:, :], inv_low[NB:, :]), 1, 1),
            ],
            axis=1,
        )
        for n, start in enumerate(starts):
            panel_ref[pl.ds(start, PIECE), :] = panel[n * PIECE : n * PIECE + PIECE]
        return carry

    lax.fori_loop(0, 2, panel_step, 0)

    for side, part_ref in enumerate((part_other_ref, part_own_ref)):
        starts = starts_of((1 - k, k)[side])
        left = left_ref[side * HALF : side * HALF + HALF, :]
        left_sq = jnp.sum(left * left, axis=1, keepdims=True)
        block = matern(left_sq, col_lane, dot3(split(left), whole(cols), 1, 1))
        panel = jnp.concatenate([panel_ref[pl.ds(start, PIECE), :] for start in starts], axis=0)
        diag = jnp.concatenate([targets_ref[pl.ds(start, PIECE), :] for start in starts], axis=0)
        total = dot3(split(block), whole(goal), 1, 0) + diag * same - dot3(split(panel), weights, 1, 0)
        part_ref[...] = total.reshape(4, 2, PIECE, NT)


def per_device(archive, slab_index, targets):
    row_place = lax.axis_index("row")
    col_place = lax.axis_index("col")
    y, z = row_place // 4, row_place % 4
    h, x, k = col_place // 8, col_place // 2 % 4, col_place % 2
    shard = archive.shape[0]
    smem = pl.BlockSpec(memory_space=pltpu.SMEM)
    vmem = pl.BlockSpec(memory_space=pltpu.VMEM)
    f32, bf16 = jnp.float32, jnp.bfloat16

    def array(kind, *shape):
        return jax.ShapeDtypeStruct(shape, kind)

    def near(array):
        return pltpu.with_memory_space_constraint(array, pltpu.VMEM)

    def call(kernel, name, outs, scratch, place, *args):
        return pl.pallas_call(
            kernel,
            out_shape=tuple(s if far else pltpu.VMEM(s.shape, s.dtype) for s, far in outs),
            in_specs=([] if place is None else [smem]) + [vmem] * len(args),
            out_specs=tuple(vmem for _ in outs),
            scratch_shapes=[pltpu.VMEM(s.shape, s.dtype) for s in scratch],
            compiler_params=pltpu.CompilerParams(vmem_limit_bytes=(40 if name == "slab" else 16) << 20),
        )(*([] if place is None else [place]), *args)

    def three(shift):
        received = []
        for s in (1, 2, 3):
            received.append(shift(s))
        return received

    place = jnp.stack([y, z, h, x, k, row_place, col_place]).astype(jnp.int32)

    stored = slab_index.reshape(TILES, SIDE, NB).transpose(1, 0, 2).reshape(SIDE, LOCAL)
    wanted = lax.dynamic_slice_in_dim(stored, col_place * PIECE, PIECE, 1).reshape(2, 2, 2, 2, PIECE)
    for axis, bit in enumerate((y // 2, y % 2, z // 2, z % 2)):
        wanted = jnp.where(bit == 1, jnp.flip(wanted, axis), wanted)
    lead_ids = lax.dynamic_slice_in_dim(stored[:PANELS, :NB].reshape(-1), (x * 2 + k) * LEAD_PIECE, LEAD_PIECE, 0)
    ids = jnp.concatenate([lead_ids, wanted.reshape(-1)]) - row_place * shard
    inside = (ids >= 0) & (ids < shard)
    picked = jnp.take(archive, jnp.clip(ids, 0, shard - 1), axis=0)
    picked = jnp.where(inside[:, None], picked, 0.0)

    early = picked[:LEAD_PIECE]
    lead = early + sum(three(lambda s: row_swap(early, s, 0)))
    lead_sum = lead
    lead = lead + sum(three(lambda s: row_swap(lead_sum, 0, s)))
    lead_own = jnp.stack([lead] + three(lambda s: col_swap(lead, 0, s, 0)))
    lead_other = col_swap(lead_own, 0, 0, 1)

    picked = picked[LEAD_PIECE:].reshape(4, 4, PIECE, F)
    mine = picked[0] + sum(three(lambda s: row_swap(picked[s], s, 0)))
    piece = mine[0] + sum(three(lambda s: row_swap(mine[s], 0, s)))

    pair = jnp.stack([piece, col_swap(piece, 1, 0, 0)])
    rows_own = jnp.stack([pair] + three(lambda s: col_swap(pair, 0, s, 0)))
    rows_other = col_swap(rows_own, 0, 0, 1)
    turned = flip(piece)
    quarter = jnp.stack([turned] + three(lambda s: row_swap(turned, 0, s)))
    cols = [quarter] + three(lambda s: row_swap(quarter, s, 0))

    square = (array(f32, LEAD, LEAD), False)
    lead_all, inverse = call(
        gram_kernel, "gram", ((array(f32, LEAD, F), False), square), (), place, near(lead_own), near(lead_other)
    )
    for first in (0, LEAD // 2):
        (inverse,) = call(
            functools.partial(factor_kernel, first), f"factor{first}", (square,), (), None, near(inverse)
        )
    panels, part_other, part_own = call(
        slab_kernel,
        "slab",
        (
            (array(f32, LOCAL, LEAD), True),
            (array(f32, 4, 2, PIECE, NT), False),
            (array(f32, 4, 2, PIECE, NT), False),
        ),
        (array(f32, LOCAL, F), array(f32, LOCAL, F))
        + (array(bf16, LOCAL, F),) * 4
        + (array(bf16, LEAD, F),) * 2
        + (array(bf16, LEAD, LEAD),) * 2,
        place, near(rows_own), near(rows_other), *(near(c) for c in cols), near(lead_all), near(inverse), targets,
    )

    total = part_own + col_swap(part_other, 0, 0, 1)
    result = total[0] + sum(three(lambda s: col_swap(total[s], 0, s, 0)))
    result = result[0] + col_swap(result[1], 1, 0, 0)
    return (panels, result)


def solution(mesh):
    placed = (P("row", None), P(), P("col", None))
    return jax.shard_map(
        per_device,
        mesh=mesh,
        in_specs=placed,
        out_specs=(P("row", None), P(("row", "col"), None)),
        check_vma=False,
    )
```
